32 devices in a mesh: dp: 8 (over z, x), section: 4 (over y, core).
Axes of the slice: x: 2, y: 2, z: 4, core: 2. Of those that a mesh axis runs over, the one named last changes fastest.
Arguments:
- hidden_in: bfloat16 [4, 4, 8, 96, 2048], P('section', None, 'dp'), may hold values from -170 to 170
- queries: bfloat16 [4, 4, 8, 96, 2048], P('section', None, 'dp'), may hold values from -96 to 96
- keys: bfloat16 [4, 4, 8, 96, 2048], P('section', None, 'dp'), may hold values from -6 to 6
- values: bfloat16 [4, 4, 8, 96, 2048], P('section', None, 'dp'), may hold values from -6 to 6
- cotangent: bfloat16 [4, 8, 96, 2048], P(None, 'dp'), may hold values from -6 to 6
- norm_gain: float32 [4, 2048], P('section'), may hold values from 0.1 to 1.9
- w_query: bfloat16 [4, 2048, 2048], P('section', 'dp'), may hold values from -0.125 to 0.125
- w_key: bfloat16 [4, 2048, 2048], P('section', 'dp'), may hold values from -0.125 to 0.125
- w_value: bfloat16 [4, 2048, 2048], P('section', 'dp'), may hold values from -0.125 to 0.125
- down_q: bfloat16 [4, 16, 2048], P('section'), may hold values from -0.125 to 0.125
- up_q: bfloat16 [4, 16, 2048], P('section'), may hold values from -0.75 to 0.75
- down_v: bfloat16 [4, 16, 2048], P('section'), may hold values from -0.125 to 0.125
- up_v: bfloat16 [4, 16, 2048], P('section'), may hold values from -0.75 to 0.75
Outputs:
- input_grad: bfloat16 [4, 4, 8, 96, 2048], P('section', None, 'dp')
- grad_down_q: float32 [4, 16, 2048], P('section')
- grad_up_q: float32 [4, 16, 2048], P('section')
- grad_down_v: float32 [4, 16, 2048], P('section')
- grad_up_v: float32 [4, 16, 2048], P('section')
The draws below stay inside these ranges and needn't reach their ends.
All inputs are finite; a program needn't handle non-finite values.
Results may differ from the reference program's by a relative error of at most 0.025.
Values may be sent and summed in bfloat16 or wider, within the bound.
A program may use at most 128 MiB of HBM per device.

```python
import jax
import jax.numpy as jnp
from jax import lax

HEADS = 16
HEAD_DIM = 128
D = 2048
RANK = 16
MICRO = 4
SEQ = 96
LAYERS = 4
BATCH = 8


def attention_pair(key):
    full_shape = (LAYERS, MICRO, BATCH, SEQ, HEADS, HEAD_DIM)
    first = jax.random.normal(jax.random.fold_in(key, 11), full_shape, jnp.float32)
    second = jax.random.normal(jax.random.fold_in(key, 23), full_shape, jnp.float32)
    query = jnp.clip(first, -6.0, 6.0)
    keyed = jnp.clip(second, -6.0, 6.0)
    final_shape = (LAYERS, MICRO, BATCH, SEQ, HEADS * HEAD_DIM)
    return (query.reshape(final_shape), keyed.reshape(final_shape))


def draw_queries(key, part):
    return attention_pair(key)[0].astype(jnp.bfloat16)


def draw_keys(key, part):
    return attention_pair(key)[1].astype(jnp.bfloat16)


def draw_hidden_in(key, part):
    full_shape = (LAYERS, MICRO, BATCH, SEQ, D)
    base = jnp.clip(jax.random.normal(jax.random.fold_in(key, 41), full_shape, jnp.float32), -6.0, 6.0)
    return base.astype(jnp.bfloat16)


def level_of(stream_key, dims, shards, low, high):
    gain, own = 1.0, jax.random.fold_in(stream_key, 6)
    for axis_at, blocks in shards:
        steps = jnp.exp(jax.random.uniform(jax.random.fold_in(own, axis_at), (blocks,), jnp.float32, low / len(shards), high / len(shards)))
        gain = gain * jnp.repeat(steps, dims[axis_at] // blocks).reshape([-1 if axis == axis_at else 1 for axis in range(len(dims))])
    return gain


def normal_values(rng, shape, deviation, bound, cuts=(), kind=jnp.bfloat16):
    gain = level_of(rng, shape, cuts, -0.22, 0.18) if cuts else 1.0
    drawn = jax.random.normal(rng, shape, jnp.float32) * deviation * gain
    return jnp.minimum(jnp.maximum(drawn, -bound), bound).astype(kind)


def setup_inputs(seed: int = 0) -> dict:
    splits = jax.random.split(jax.random.key(seed), 14)
    hidden_in = draw_hidden_in(jax.random.fold_in(splits[13], 71), 0)
    queries = draw_queries(jax.random.fold_in(splits[13], 71), 0)
    keys = draw_keys(jax.random.fold_in(splits[13], 71), 0)
    values = normal_values(splits[3], (LAYERS, MICRO, BATCH, SEQ, D), 1.0, 6.0, ((0, 4), (2, 8)))
    cotangent = normal_values(splits[4], (MICRO, BATCH, SEQ, D), 1.0, 6.0, ((1, 8),))
    norm_gain = jnp.clip(1.0 + 0.18 * jax.random.normal(splits[5], (LAYERS, D), jnp.float32), 0.1, 1.9)
    w_query = normal_values(splits[6], (LAYERS, D, D), D ** -0.5, 0.125, ((0, 4), (1, 8)))
    w_key = normal_values(splits[7], (LAYERS, D, D), D ** -0.5, 0.125, ((0, 4), (1, 8)))
    w_value = normal_values(splits[8], (LAYERS, D, D), D ** -0.5, 0.125, ((0, 4), (1, 8)))
    down_q = normal_values(splits[9], (LAYERS, RANK, D), D ** -0.5, 0.125, ((0, 4),))
    up_q = normal_values(splits[10], (LAYERS, RANK, D), (4 * RANK) ** -0.5, 0.75, ((0, 4),))
    down_v = normal_values(splits[11], (LAYERS, RANK, D), D ** -0.5, 0.125, ((0, 4),))
    up_v = normal_values(splits[12], (LAYERS, RANK, D), (4 * RANK) ** -0.5, 0.75, ((0, 4),))
    return {"hidden_in": hidden_in, "queries": queries, "keys": keys, "values": values, "cotangent": cotangent, "norm_gain": norm_gain, "w_query": w_query, "w_key": w_key, "w_value": w_value, "down_q": down_q, "up_q": up_q, "down_v": down_v, "up_v": up_v}


adapter_scale = 2.0
norm_eps = 1e-05

def input_backward(hidden, query, keyed, valued, out_grad, gain_row, frozen, adapter_weights):
    count, positions, features = hidden.shape
    head_count = features // HEAD_DIM
    scale = HEAD_DIM ** (-0.5)
    floated = hidden.astype(jnp.float32)
    inverse = lax.rsqrt(lax.optimization_barrier(jnp.mean(floated * floated, axis=-1, keepdims=True)) + norm_eps)
    normed = (floated * inverse * gain_row).astype(jnp.bfloat16)
    split = (count, positions, head_count, HEAD_DIM)
    query_heads = query.astype(jnp.float32).reshape(split)
    key_heads = keyed.astype(jnp.float32).reshape(split)
    value_heads = valued.astype(jnp.float32).reshape(split)
    grad_heads = out_grad.astype(jnp.float32).reshape(split)
    scores = jnp.einsum('nqhd,nkhd->nhqk', query_heads, key_heads) * scale
    causal = lax.broadcasted_iota(jnp.int32, (positions, positions), 1) <= lax.broadcasted_iota(jnp.int32, (positions, positions), 0)
    scores = jnp.where(causal, scores, -1e+30)
    attend = jax.nn.softmax(scores, axis=-1)
    attend_low = lax.optimization_barrier(attend.astype(jnp.bfloat16)).astype(jnp.float32)
    attend_grad = jnp.einsum('nqhd,nkhd->nhqk', grad_heads, value_heads)
    value_grad = jnp.einsum('nhqk,nqhd->nkhd', attend_low, grad_heads).astype(jnp.bfloat16)
    row_total = lax.optimization_barrier(jnp.sum(attend * attend_grad, axis=-1, keepdims=True))
    score_grad = (attend * (attend_grad - row_total) * scale).astype(jnp.bfloat16)
    score_wide = lax.optimization_barrier(score_grad).astype(jnp.float32)
    query_grad = jnp.einsum('nhqk,nkhd->nqhd', score_wide, key_heads).astype(jnp.bfloat16)
    key_grad = jnp.einsum('nhqk,nqhd->nkhd', score_wide, query_heads).astype(jnp.bfloat16)
    rows = count * positions
    flattened_query = query_grad.reshape(rows, features)
    key_flat = key_grad.reshape(rows, features)
    flattened_value = value_grad.reshape(rows, features)
    contract_matrices = (((1,), (1,)), ((), ()))
    normed_grad = lax.dot_general(flattened_query, frozen[0], contract_matrices, preferred_element_type=jnp.float32)
    normed_grad = normed_grad + lax.dot_general(key_flat, frozen[1], contract_matrices, preferred_element_type=jnp.float32)
    normed_grad = normed_grad + lax.dot_general(flattened_value, frozen[2], contract_matrices, preferred_element_type=jnp.float32)
    query_low_rank = (adapter_scale * lax.dot_general(flattened_query, adapter_weights[1], contract_matrices, preferred_element_type=jnp.float32)).astype(jnp.bfloat16)
    value_low_rank = (adapter_scale * lax.dot_general(flattened_value, adapter_weights[3], contract_matrices, preferred_element_type=jnp.float32)).astype(jnp.bfloat16)
    normed_grad = normed_grad + jnp.dot(query_low_rank, adapter_weights[0], preferred_element_type=jnp.float32)
    normed_grad = normed_grad + jnp.dot(value_low_rank, adapter_weights[2], preferred_element_type=jnp.float32)
    scaled_grad = (gain_row * normed_grad).reshape(count, positions, features)
    correction = lax.optimization_barrier(jnp.mean(floated * scaled_grad, axis=-1, keepdims=True))
    input_grad = (out_grad.astype(jnp.float32) + inverse * scaled_grad - floated * inverse ** 3 * correction).astype(jnp.bfloat16)
    saved = (normed.reshape(rows, features), flattened_query, flattened_value, query_low_rank, value_low_rank)
    return (input_grad, saved)

def adapter_grads(normed, flattened_query, flattened_value, query_low_rank, value_low_rank, down_query, down_value):
    contract_matrices = (((1,), (1,)), ((), ()))
    across_replicas_total = (((0,), (0,)), ((), ()))
    normalized_query = lax.dot_general(normed, down_query, contract_matrices, preferred_element_type=jnp.float32).astype(jnp.bfloat16)
    normalized_value = lax.dot_general(normed, down_value, contract_matrices, preferred_element_type=jnp.float32).astype(jnp.bfloat16)
    grad_dq = lax.dot_general(query_low_rank, normed, across_replicas_total, preferred_element_type=jnp.float32)
    query_up_gradient = adapter_scale * lax.dot_general(normalized_query, flattened_query, across_replicas_total, preferred_element_type=jnp.float32)
    grad_dv = lax.dot_general(value_low_rank, normed, across_replicas_total, preferred_element_type=jnp.float32)
    value_up_gradient = adapter_scale * lax.dot_general(normalized_value, flattened_value, across_replicas_total, preferred_element_type=jnp.float32)
    return (grad_dq, query_up_gradient, grad_dv, value_up_gradient)

def reference(hidden_in, queries, keys, values, cotangent, norm_gain, w_query, w_key, w_value, down_q, up_q, down_v, up_v):
    count = MICRO * BATCH
    out_grad = cotangent.reshape(count, SEQ, D)
    input_list = []
    grad_lists = ([], [], [], [])
    for current in reversed(range(LAYERS)):
        frozen = (w_query[current], w_key[current], w_value[current])
        adapter_weights = (down_q[current], up_q[current], down_v[current], up_v[current])
        input_grad, saved = input_backward(hidden_in[current].reshape(count, SEQ, D), queries[current].reshape(count, SEQ, D), keys[current].reshape(count, SEQ, D), values[current].reshape(count, SEQ, D), out_grad, norm_gain[current], frozen, adapter_weights)
        totals = adapter_grads(*saved, adapter_weights[0], adapter_weights[2])
        input_list.append(input_grad)
        for target, total in zip(grad_lists, totals):
            target.append(total)
        out_grad = input_grad
    ordered = input_list[::-1]
    scale = (MICRO * BATCH * SEQ) ** (-0.5)
    stacked = [jnp.stack(target[::-1]) * scale for target in grad_lists]
    input_all = jnp.stack(ordered).reshape(LAYERS, MICRO, BATCH, SEQ, D)
    return (input_all, stacked[0], stacked[1], stacked[2], stacked[3])
```

```python
import jax
import jax.numpy as jnp
from jax import lax
from jax.sharding import PartitionSpec as P

HEAD_DIM = 128
adapter_scale = 2.0
norm_eps = 1e-05
NT = (((1,), (1,)), ((), ()))
TN = (((0,), (0,)), ((), ()))
F32 = jnp.float32
BF16 = jnp.bfloat16


def dot(a, b, dims):
    return lax.dot_general(a, b, dims, preferred_element_type=F32)


def swap(value, axis, bit):
    n = lax.axis_size(axis)
    return lax.ppermute(value, axis, [(i, i ^ bit) for i in range(n)])


def total_over(value, axis, sent):
    bit = 1
    while bit < lax.axis_size(axis):
        value = value + swap(value.astype(sent), axis, bit).astype(F32)
        bit *= 2
    return value


def spread(columns, owner, axis):
    n = lax.axis_size(axis)
    me = lax.axis_index(axis)
    width = columns.shape[-1] // n
    block = columns[..., owner * width : (owner + 1) * width]
    for k in range(1, n):
        j = (owner + k) % n
        got = lax.ppermute(columns[..., j * width : (j + 1) * width], axis, [(owner, j)])
        block = jnp.where(me == j, got, block)
    return block


def collect(block, owner, axis):
    n = lax.axis_size(axis)
    parts = [block if j == owner else lax.ppermute(block, axis, [(j, owner)]) for j in range(n)]
    return jnp.concatenate(parts, axis=-1)


def after(value, token):
    return value if token is None else lax.optimization_barrier((value, token))[0]


def gather_rows(shard):
    n = lax.axis_size("dp")
    if n % 2 or n > 8 or shard.shape[0] % 64:
        whole = lax.all_gather(shard, "dp", axis=0, tiled=True)
        return whole, whole[:8]
    line = n // 2
    d = lax.axis_index("dp")
    z = d // 2
    rows, width = shard.shape
    early = rows * 3 // 16 // 16 * 16
    late = rows - early
    whole = jnp.zeros((n + 2, rows, width), BF16)
    own = shard[:late]
    pair = shard[late:]

    def put(whole, piece, slot, valid, start):
        at = n if valid is None else jnp.where(valid, slot, n)
        at = slot if valid is None else at
        return lax.dynamic_update_slice(whole, piece, (at, start, 0))

    whole = put(whole, own[None], d, None, 0)
    other = lax.ppermute(own, "dp", [(i, i ^ 1) for i in range(n)])
    whole = put(whole, other[None], d ^ 1, None, 0)
    mate = lax.ppermute(pair, "dp", [(i, i ^ 1) for i in range(n)])
    first = d % 2 == 0
    both = jnp.stack([jnp.where(first, pair, mate), jnp.where(first, mate, pair)])
    whole = put(whole, both, 2 * z, None, late)
    lanes = {1: (own, both), -1: (own, both)}
    token = mate
    for k in range(1, line):
        if k == line - 1:
            token = (lanes[1][1], lanes[-1][1])
        for way in (1, -1):
            held, held_both = lanes[way]
            holds = [p for p in range(line) if 0 <= p - way * (k - 1) < line]
            route = [(p * 2 + x, (p + way) * 2 + x) for p in holds if 0 <= p + way < line for x in (0, 1)]
            held = lax.ppermute(held, "dp", route)
            held_both = lax.ppermute(held_both, "dp", route)
            lanes[way] = (held, held_both)
            across = lax.ppermute(held, "dp", [(b, b ^ 1) for _, b in route])
            source = z - way * k
            valid = (source >= 0) & (source < line)
            slot = d - 2 * way * k
            whole = put(whole, held[None], slot, valid, 0)
            whole = put(whole, across[None], slot + 1 - 2 * (d % 2), valid, 0)
            whole = put(whole, held_both, 2 * source, valid, late)
    return whole.reshape((n + 2) * rows, width), token


def on_device(hidden_in, queries, keys, values, cotangent, norm_gain, w_query, w_key, w_value, down_q, up_q, down_v, up_v):
    layers = lax.axis_size("section")
    me = lax.axis_index("section")
    micro, positions, features = cotangent.shape[0], cotangent.shape[2], cotangent.shape[3]
    rows = micro * positions
    width = features // layers
    rank = down_q.shape[1]

    def mine(value):
        return lax.dynamic_slice_in_dim(value, me * width, width, value.ndim - 1)

    weights = jnp.stack([w_query[0], w_key[0], w_value[0]])
    hidden_full = hidden_in.reshape(rows, features)
    acts = jnp.stack([hidden_full, queries.reshape(rows, features), keys.reshape(rows, features), values.reshape(rows, features)])
    floated = hidden_full.astype(F32)
    squares = jnp.mean(floated * floated, axis=-1)
    stats = lax.all_gather(jnp.concatenate([norm_gain[0], squares]), "section")
    adapters = lax.all_gather(jnp.concatenate([down_q[0], down_v[0], up_q[0], up_v[0]]), "section")

    causal = lax.broadcasted_iota(jnp.int32, (positions, positions), 1) <= lax.broadcasted_iota(
        jnp.int32, (positions, positions), 0
    )
    scale = HEAD_DIM ** (-0.5)
    split = (micro, positions, width // HEAD_DIM, HEAD_DIM)
    sections, shards, gathered = {}, {}, {}
    w_token = a_token = None
    for l in reversed(range(layers)):
        block = spread(after(weights, w_token), l, "section")
        w_token = block
        a_token = block if a_token is None else a_token
        sections[l] = spread(after(acts, a_token), l, "section")
        a_token = sections[l]
        shards[l] = jnp.concatenate([block[0], block[1], block[2]], axis=-1)
    token = None
    for l in reversed(range(layers)):
        gathered[l], token = gather_rows(after(shards[l], token))

    out_grad = mine(cotangent.reshape(rows, features))
    final_input = None
    final_grads = None
    for l in reversed(range(layers)):
        hidden, query, keyed, valued = sections[l]
        gain = stats[l, :features]
        gain_mine = mine(gain)[None]
        inverse = lax.rsqrt(stats[l, features:] + norm_eps)[:, None]
        hidden_f = hidden.astype(F32)
        normed = (hidden_f * inverse * gain_mine).astype(BF16)
        down, up = adapters[l, : 2 * rank], adapters[l, 2 * rank :]
        up_mine = mine(up)
        low_normed = dot(normed, mine(down), NT)

        qh, kh, vh = query.reshape(split), keyed.reshape(split), valued.reshape(split)
        gh = out_grad.reshape(split)
        scores = jnp.einsum("nqhd,nkhd->nhqk", qh, kh, preferred_element_type=F32) * scale
        attend = jax.nn.softmax(jnp.where(causal, scores, -1e30), axis=-1)
        attend_grad = jnp.einsum("nqhd,nkhd->nhqk", gh, vh, preferred_element_type=F32)
        value_grad = jnp.einsum("nhqk,nqhd->nkhd", attend.astype(BF16), gh, preferred_element_type=F32)
        row_total = jnp.sum(attend * attend_grad, axis=-1, keepdims=True)
        score_grad = (attend * (attend_grad - row_total) * scale).astype(BF16)
        query_grad = jnp.einsum("nhqk,nkhd->nqhd", score_grad, kh, preferred_element_type=F32)
        key_grad = jnp.einsum("nhqk,nqhd->nkhd", score_grad, qh, preferred_element_type=F32)
        qg = query_grad.astype(BF16).reshape(rows, width)
        kg = key_grad.astype(BF16).reshape(rows, width)
        vg = value_grad.astype(BF16).reshape(rows, width)

        low = adapter_scale * jnp.concatenate(
            [dot(qg, up_mine[:rank], NT), dot(vg, up_mine[rank:], NT)], axis=-1
        )
        part = dot(jnp.concatenate([qg, kg, vg], axis=-1), gathered[l], NT)[:, :features]
        part = part + jnp.dot(low.astype(BF16), down, preferred_element_type=F32)
        blocks = [part[:, j * width : (j + 1) * width] for j in range(layers)]
        bit = 1
        while bit < layers:
            upper = (me & bit) != 0
            keep = [jnp.where(upper, b, a) for a, b in zip(blocks[::2], blocks[1::2])]
            send = [jnp.where(upper, a, b).astype(BF16) for a, b in zip(blocks[::2], blocks[1::2])]
            got = swap(jnp.concatenate(send, axis=-1), "section", bit)
            blocks = [k + got[:, j * width : (j + 1) * width].astype(F32) for j, k in enumerate(keep)]
            bit *= 2
        scaled = gain_mine * blocks[0]
        correction = total_over(jnp.sum(hidden_f * scaled, axis=-1), "section", F32)[:, None] / features
        input_grad = (
            out_grad.astype(F32) + inverse * scaled - hidden_f * inverse**3 * correction
        ).astype(BF16)
        input_whole = collect(input_grad, l, "section")
        out_grad = input_grad

        lows = total_over(jnp.concatenate([low, low_normed], axis=-1), "section", F32).astype(BF16)
        grad_down = dot(lows[:, : 2 * rank], normed, TN)
        grad_up_q = adapter_scale * dot(lows[:, 2 * rank : 3 * rank], qg, TN)
        grad_up_v = adapter_scale * dot(lows[:, 3 * rank :], vg, TN)
        grads = total_over(jnp.concatenate([grad_down, grad_up_q, grad_up_v]), "dp", BF16)
        grads_whole = collect(grads, l, "section")
        if final_input is None:
            final_input, final_grads = input_whole, grads_whole
        else:
            final_input = jnp.where(me == l, input_whole, final_input)
            final_grads = jnp.where(me == l, grads_whole, final_grads)

    s = (rows * cotangent.shape[1] * lax.axis_size("dp")) ** (-0.5)
    final_grads = final_grads * s
    return (
        final_input.reshape(1, micro, 1, positions, features),
        final_grads[None, :rank],
        final_grads[None, 2 * rank : 3 * rank],
        final_grads[None, rank : 2 * rank],
        final_grads[None, 3 * rank :],
    )


def solution(mesh):
    rows = P("section", None, "dp", None, None)
    cut = P("section", "dp", None)
    small = P("section", None, None)
    return jax.shard_map(
        on_device,
        mesh=mesh,
        in_specs=(rows,) * 4 + (P(None, "dp", None, None), P("section", None)) + (cut,) * 3 + (small,) * 4,
        out_specs=(rows,) + (small,) * 4,
        check_vma=False,
    )
```

```python
import jax
import jax.numpy as jnp
from jax import lax
from jax.sharding import PartitionSpec as P

HEAD_DIM = 128
adapter_scale = 2.0
norm_eps = 1e-05
NT = (((1,), (1,)), ((), ()))
TN = (((0,), (0,)), ((), ()))
F32 = jnp.float32
BF16 = jnp.bfloat16


def dot(a, b, dims):
    return lax.dot_general(a, b, dims, preferred_element_type=F32)


def swap(value, axis, bit):
    n = lax.axis_size(axis)
    return lax.ppermute(value, axis, [(i, i ^ bit) for i in range(n)])


def total_over(value, axis, sent):
    bit = 1
    while bit < lax.axis_size(axis):
        value = value + swap(value.astype(sent), axis, bit).astype(F32)
        bit *= 2
    return value


def exchange(pieces, axis):
    n = lax.axis_size(axis)
    me = lax.axis_index(axis)
    got = [lax.dynamic_index_in_dim(pieces, me, 0, False)]
    for k in range(1, n):
        sent = lax.dynamic_index_in_dim(pieces, lax.rem(me + k, n), 0, False)
        got.append(lax.ppermute(sent, axis, [(i, (i + k) % n) for i in range(n)]))
    return lambda j: pick(got, lax.rem(me + n - j, n))


def pick(choices, index):
    value = choices[0]
    for k, choice in enumerate(choices[1:], 1):
        value = jnp.where(index == k, choice, value)
    return value


def on_device(hidden_in, queries, keys, values, cotangent, norm_gain, w_query, w_key, w_value, down_q, up_q, down_v, up_v):
    layers = lax.axis_size("section")
    me = lax.axis_index("section")
    micro, positions, features = cotangent.shape[0], cotangent.shape[2], cotangent.shape[3]
    rows = micro * positions
    width = features // layers
    rank = down_q.shape[1]

    def mine(value):
        return lax.dynamic_slice_in_dim(value, me * width, width, value.ndim - 1)

    hidden_full = hidden_in.reshape(rows, features)
    acts = jnp.stack([hidden_full, queries.reshape(rows, features), keys.reshape(rows, features), values.reshape(rows, features)])
    floated = hidden_full.astype(F32)
    squares = jnp.mean(floated * floated, axis=-1)
    stats = lax.all_gather(jnp.concatenate([norm_gain[0], squares]), "section")
    adapters = lax.all_gather(jnp.concatenate([down_q[0], down_v[0], up_q[0], up_v[0]]), "section")

    causal = lax.broadcasted_iota(jnp.int32, (positions, positions), 1) <= lax.broadcasted_iota(
        jnp.int32, (positions, positions), 0
    )
    scale = HEAD_DIM ** (-0.5)
    split = (micro, positions, width // HEAD_DIM, HEAD_DIM)
    def cut(value):
        return jnp.stack([value[..., j * width : (j + 1) * width] for j in range(layers)])

    flat = jnp.stack(
        [
            jnp.concatenate([w[0][:, j * width : (j + 1) * width] for w in (w_query, w_key, w_value)], axis=-1)
            for j in range(layers)
        ]
    )
    shard_of = exchange(flat, "section")
    gathered = {}
    for l in reversed(range(layers)):
        gathered[l] = lax.all_gather(shard_of(l), "dp", axis=0, tiled=True)
    act_of = exchange(cut(acts), "section")

    out_grad = mine(cotangent.reshape(rows, features))
    input_grads, kept = {}, {}
    for l in reversed(range(layers)):
        hidden, query, keyed, valued = act_of(l)
        gain = stats[l, :features]
        gain_mine = mine(gain)[None]
        inverse = lax.rsqrt(stats[l, features:] + norm_eps)[:, None]
        hidden_f = hidden.astype(F32)
        normed = (hidden_f * inverse * gain_mine).astype(BF16)
        down, up = adapters[l, : 2 * rank], adapters[l, 2 * rank :]
        up_mine = mine(up)
        low_normed = dot(normed, mine(down), NT)

        qh, kh, vh = query.reshape(split), keyed.reshape(split), valued.reshape(split)
        gh = out_grad.reshape(split)
        scores = jnp.einsum("nqhd,nkhd->nhqk", qh, kh, preferred_element_type=F32) * scale
        attend = jax.nn.softmax(jnp.where(causal, scores, -1e30), axis=-1)
        attend_grad = jnp.einsum("nqhd,nkhd->nhqk", gh, vh, preferred_element_type=F32)
        value_grad = jnp.einsum("nhqk,nqhd->nkhd", attend.astype(BF16), gh, preferred_element_type=F32)
        row_total = jnp.sum(attend * attend_grad, axis=-1, keepdims=True)
        score_grad = (attend * (attend_grad - row_total) * scale).astype(BF16)
        query_grad = jnp.einsum("nhqk,nkhd->nqhd", score_grad, kh, preferred_element_type=F32)
        key_grad = jnp.einsum("nhqk,nqhd->nkhd", score_grad, qh, preferred_element_type=F32)
        qg = query_grad.astype(BF16).reshape(rows, width)
        kg = key_grad.astype(BF16).reshape(rows, width)
        vg = value_grad.astype(BF16).reshape(rows, width)

        low = adapter_scale * jnp.concatenate(
            [dot(qg, up_mine[:rank], NT), dot(vg, up_mine[rank:], NT)], axis=-1
        )
        part = dot(jnp.concatenate([qg, kg, vg], axis=-1), gathered[l], NT)
        part = part + jnp.dot(low.astype(BF16), down, preferred_element_type=F32)
        blocks = [part[:, j * width : (j + 1) * width] for j in range(layers)]
        bit = 1
        while bit < layers:
            upper = (me & bit) != 0
            keep = [jnp.where(upper, b, a) for a, b in zip(blocks[::2], blocks[1::2])]
            send = [jnp.where(upper, a, b).astype(BF16) for a, b in zip(blocks[::2], blocks[1::2])]
            got = swap(jnp.concatenate(send, axis=-1), "section", bit)
            blocks = [k + got[:, j * width : (j + 1) * width].astype(F32) for j, k in enumerate(keep)]
            bit *= 2
        scaled = gain_mine * blocks[0]
        correction = total_over(jnp.sum(hidden_f * scaled, axis=-1), "section", F32)[:, None] / features
        input_grad = (
            out_grad.astype(F32) + inverse * scaled - hidden_f * inverse**3 * correction
        ).astype(BF16)
        out_grad = input_grad
        input_grads[l] = input_grad
        kept[l] = (jnp.concatenate([low, low_normed], axis=-1), normed, qg, vg)

    input_of = exchange(jnp.stack([input_grads[l] for l in range(layers)]), "section")
    final_input = jnp.concatenate([input_of(j) for j in range(layers)], axis=-1)
    lows_all = total_over(jnp.stack([kept[l][0] for l in range(layers)]), "section", F32).astype(BF16)
    grads = []
    for l in range(layers):
        lows = lows_all[l]
        _, normed, qg, vg = kept[l]
        grad_down = dot(lows[:, : 2 * rank], normed, TN)
        grad_up_q = adapter_scale * dot(lows[:, 2 * rank : 3 * rank], qg, TN)
        grad_up_v = adapter_scale * dot(lows[:, 3 * rank :], vg, TN)
        grads.append(jnp.concatenate([grad_down, grad_up_q, grad_up_v]))
    grads = total_over(jnp.stack(grads), "dp", BF16)
    grad_of = exchange(grads, "section")
    final_grads = jnp.concatenate([grad_of(j) for j in range(layers)], axis=-1)

    s = (rows * cotangent.shape[1] * lax.axis_size("dp")) ** (-0.5)
    final_grads = final_grads * s
    return (
        final_input.reshape(1, micro, 1, positions, features),
        final_grads[None, :rank],
        final_grads[None, 2 * rank : 3 * rank],
        final_grads[None, rank : 2 * rank],
        final_grads[None, 3 * rank :],
    )


def solution(mesh):
    rows = P("section", None, "dp", None, None)
    cut = P("section", "dp", None)
    small = P("section", None, None)
    return jax.shard_map(
        on_device,
        mesh=mesh,
        in_specs=(rows,) * 4 + (P(None, "dp", None, None), P("section", None)) + (cut,) * 3 + (small,) * 4,
        out_specs=(rows,) + (small,) * 4,
        check_vma=False,
    )
```
